128 devices in a mesh: freq: 4 (over y), pts: 32 (over z, x, core).
Axes of the slice: x: 4, y: 4, z: 4, core: 2. Of those that a mesh axis runs over, the one named last changes fastest.
Arguments:
- data: float32 [2, 32, 64, 3, 32768], P(None, 'freq', None, None, 'pts'), may hold values from -180 to 180
- quad_weight: float32 [32768], P('pts'), may hold values from 0.2 to 5
- basis: float32 [2, 32, 64, 8], P(None, 'freq'), may hold values from -6 to 6
Outputs:
- basis_out: float32 [2, 32, 64, 8], P(None, 'freq')
- spectrum: float32 [32, 8], P('freq')
- modes: float32 [2, 32, 8, 3, 32768], P(None, 'freq', None, None, 'pts')
The draws below stay inside these ranges and needn't reach their ends.
All inputs are finite; a program needn't handle non-finite values.
Results may differ from the reference program's by a relative error of at most 0.0001.
Values sent between devices are 32-bit elements; how exact they have to be, the bound alone decides.
A program may use at most 128 MiB of HBM per device.

```python
import math
import jax
import jax.numpy as jnp
from jax import lax

BLOCKS = 64
RANK = 8
COMP = 3
ITERS = 4
FREQ_ALL = 32
NPTS = 32768


def draw_data(key, part):
    first, second = jax.random.split(key, 2)
    shape = (2, FREQ_ALL, BLOCKS, COMP, NPTS)
    ramp = 1.0 + 2.0 * jnp.arange(FREQ_ALL, dtype=jnp.float32) / max(FREQ_ALL - 1, 1)
    block_scale = jnp.exp(jax.random.uniform(second, (FREQ_ALL, BLOCKS), jnp.float32, 0.0, math.log(10.0)))
    values = jnp.clip(jax.random.normal(first, shape, jnp.float32), -6.0, 6.0)
    scaled = values * (ramp[:, None] * block_scale)[None, :, :, None, None]
    return scaled.astype(jnp.float32)


def level_of(key, dims, pieces, smallest, high):
    factor_of = 1.0
    for axis_at, parts in pieces:
        heights = jax.random.uniform(jax.random.fold_in(jax.random.fold_in(key, 6), axis_at), (parts,), jnp.float32, smallest / len(pieces), high / len(pieces))
        factor_of = factor_of * jnp.repeat(jnp.exp(heights), dims[axis_at] // parts).reshape((-1,) + (1,) * (len(dims) - 1 - axis_at))
    return factor_of


def scatter_about(stream_key, dims, deviation, limit, shards=(), kind=jnp.bfloat16):
    gain = level_of(stream_key, dims, shards, -0.22, 0.18) if shards else 1.0
    result = jax.random.normal(stream_key, dims, jnp.float32) * deviation * gain
    return jnp.minimum(jnp.maximum(result, -limit), limit).astype(kind)


def setup_inputs(seed: int = 0) -> dict:
    keys = jax.random.split(jax.random.key(seed), 4)
    data = draw_data(jax.random.fold_in(keys[3], 71), 0)
    quad_weight = jnp.clip(jnp.exp(math.log(5.0) - 3.218876 * jax.random.uniform(keys[1], (NPTS,), jnp.float32) ** level_of(keys[1], (NPTS,), ((0, 32),), -0.2, 0.2)), 0.2, 5.0)
    basis = scatter_about(keys[2], (2, FREQ_ALL, BLOCKS, RANK), 1.0, 6.0, ((1, 4),), jnp.float32)
    return dict(data=data, quad_weight=quad_weight, basis=basis)


def matmul_high(left, right):
    return jnp.matmul(left, right, precision=lax.Precision.HIGHEST)

def apply_gram(gram_real, gram_imag, vec_real, vec_imag):
    out_real = matmul_high(gram_real, vec_real) - matmul_high(gram_imag, vec_imag)
    out_imag = matmul_high(gram_real, vec_imag) + matmul_high(gram_imag, vec_real)
    return (out_real, out_imag)

def orthonormalize(z_real, z_imag):
    blocks = z_real.shape[-2]
    cols_real = []
    cols_imag = []
    for column in range(z_real.shape[-1]):
        cur_real = z_real[..., column]
        cur_imag = z_imag[..., column]
        for earlier in range(column):
            base_real = cols_real[earlier]
            base_imag = cols_imag[earlier]
            coef_real = lax.optimization_barrier(jnp.sum(base_real * cur_real + base_imag * cur_imag, axis=-1)) / blocks
            coef_imag = lax.optimization_barrier(jnp.sum(base_real * cur_imag - base_imag * cur_real, axis=-1)) / blocks
            cur_real = cur_real - (coef_real[..., None] * base_real - coef_imag[..., None] * base_imag)
            cur_imag = cur_imag - (coef_real[..., None] * base_imag + coef_imag[..., None] * base_real)
        factor = lax.rsqrt(lax.optimization_barrier(jnp.mean(cur_real * cur_real + cur_imag * cur_imag, axis=-1)) + 1e-06)
        cols_real.append(cur_real * factor[..., None])
        cols_imag.append(cur_imag * factor[..., None])
    return (jnp.stack(cols_real, axis=-1), jnp.stack(cols_imag, axis=-1))

def reference(data, quad_weight, basis):
    scaling = 1.0 / (COMP * NPTS)
    weights = jnp.tile(quad_weight, COMP)

    def one_freq(index):
        block = lax.dynamic_index_in_dim(data, index, 1, keepdims=False)
        samples = block.reshape(2, BLOCKS, COMP * NPTS)
        weighted = samples * weights[None, None, :]
        gram_real = (matmul_high(samples[0], weighted[0].T) + matmul_high(samples[1], weighted[1].T)) * scaling
        gram_imag = (matmul_high(samples[0], weighted[1].T) - matmul_high(samples[1], weighted[0].T)) * scaling
        start = lax.dynamic_index_in_dim(basis, index, 1, keepdims=False)
        vec_real = start[0]
        vec_imag = start[1]
        for step in range(ITERS):
            z_real, z_imag = apply_gram(gram_real, gram_imag, vec_real, vec_imag)
            vec_real, vec_imag = orthonormalize(z_real, z_imag)
        z_real, z_imag = apply_gram(gram_real, gram_imag, vec_real, vec_imag)
        rayleigh = lax.optimization_barrier(jnp.sum(vec_real * z_real + vec_imag * z_imag, axis=-2)) / BLOCKS
        proj_real = matmul_high(vec_real.T, samples[0]) - matmul_high(vec_imag.T, samples[1])
        proj_imag = matmul_high(vec_imag.T, samples[0]) + matmul_high(vec_real.T, samples[1])
        projected = jnp.stack([proj_real, proj_imag]) / BLOCKS
        trace_value = jnp.sum(jnp.diagonal(gram_real))
        return (jnp.stack([vec_real, vec_imag]), rayleigh, projected.reshape(2, RANK, COMP, NPTS), trace_value)
    bases, rayleigh, projected, traces = lax.map(one_freq, jnp.arange(FREQ_ALL, dtype=jnp.int32))
    total = jnp.sum(traces)
    spectrum = rayleigh * (FREQ_ALL * BLOCKS) / total
    return (jnp.moveaxis(bases, 0, 1), spectrum, jnp.moveaxis(projected, 0, 1))
```

```python
import functools
import jax
import jax.numpy as jnp
from jax import lax
from jax.experimental import pallas as pl
from jax.experimental.pallas import tpu as pltpu
from jax.sharding import PartitionSpec as P

ITERS = 4
AHEAD = 3
F32 = jnp.float32
BF16 = jnp.bfloat16
MESH = pl.DeviceIdType.MESH


def split3(value):
    first = value.astype(BF16).astype(F32)
    rest = value - first
    second = rest.astype(BF16).astype(F32)
    return first, second, rest - second


def iota(shape, dim):
    return lax.broadcasted_iota(jnp.int32, shape, dim)


def kernel(
    data, weight, basis, basis_out, spec_out, modes_out,
    xbuf, ybuf, pbuf, rbuf, zbuf, tbuf, vbuf, abuf, rmat, obuf,
    load_sem, out_sem, ps_sem, pr_sem, zs_sem, zr_sem, ts_sem, tr_sem, vs_sem, vr_sem, as_sem, ar_sem,
):
    me = lax.axis_index("pts")
    line = lax.axis_index("freq")
    z = me // 8
    q = me % 8
    x = q // 2
    core = q % 2
    sign = 1 - 2 * ((3 - x) // 3)
    near = [(2, 0), (2, 1), (sign, 0), (sign, 1), (-sign, 0), (-sign, 1), (0, 1), (0, 0)]
    freq = [((x + dx + 4) % 4) * 2 + (core + dc) % 2 for dx, dc in near]
    rows = [z * 8 + f for f in freq]
    cols = [((z + d) % 4) * 8 + q for d in (2, 1, 3)]
    lines = [(line + d) % 4 for d in (2, 1, 3)]

    def load(s, part):
        return pltpu.make_async_copy(data.at[part, freq[s]], xbuf.at[s, part], load_sem.at[s, part])

    for s in range(AHEAD):
        load(s, 0).start()
        load(s, 1).start()

    barrier = pltpu.get_barrier_semaphore()
    for peer in rows[:7] + cols:
        pl.semaphore_signal(barrier, inc=1, device_id={"pts": peer}, device_id_type=MESH)
    for peer in lines:
        pl.semaphore_signal(barrier, inc=1, device_id={"freq": peer}, device_id_type=MESH)

    w = weight[...]
    root = jnp.sqrt(w)
    low = iota((1, 128), 1) < 64
    half = jnp.where(low, 1.0, -1.0).astype(F32)

    def product(s):
        load(s, 0).wait()
        load(s, 1).wait()
        if s + AHEAD < 8:
            load(s + AHEAD, 0).start()
            load(s + AHEAD, 1).start()
        for c in range(3):
            span = pl.ds(c * 1024, 1024)
            for part in range(2):
                y = xbuf[s, part, c] * root
                hi = y.astype(BF16)
                lo = (y - hi.astype(F32)).astype(BF16)
                ybuf[s, pl.ds(part * 64, 64), span] = hi
                ybuf[s, pl.ds(128 + part * 64, 64), span] = lo
        total = None
        for k in range(2):
            both = ybuf[s, :, pl.ds(k * 1536, 1536)]
            m = lax.dot_general(both, both, (((1,), (1,)), ((), ())), preferred_element_type=F32)
            total = m if total is None else total + m
        return (total[:128, :128] + total[128:, 128:]) + (total[:128, 128:] + total[128:, :128])

    def packed(m):
        top, bottom = m[:64], m[64:]
        straight = top + half * pltpu.roll(bottom, 64, 1)
        swapped = pltpu.roll(top, 64, 1) - half * bottom
        row = iota((64, 128), 0)
        col = iota((64, 128), 1) % 64
        upper = jnp.where(low == (col >= row), straight, swapped)
        return jnp.where(low, upper[:32], upper[32:])

    def send_product(s):
        return pltpu.make_async_remote_copy(
            src_ref=pbuf.at[s], dst_ref=rbuf.at[q], send_sem=ps_sem.at[s], recv_sem=pr_sem.at[q],
            device_id={"pts": rows[s]}, device_id_type=MESH)

    def take_product(s):
        return pltpu.make_async_remote_copy(
            src_ref=pbuf.at[s], dst_ref=rbuf.at[freq[s]], send_sem=ps_sem.at[s], recv_sem=pr_sem.at[freq[s]],
            device_id={"pts": rows[s]}, device_id_type=MESH)

    before = None
    for s in range(8):
        now = product(s)
        if s == 1:
            pl.semaphore_wait(barrier, 13)
        if s:
            pbuf[s - 1] = packed(before)
            send_product(s - 1).start()
        before = now
    total = packed(before)
    for s in range(7):
        take_product(s).wait_recv()
        total = total + rbuf[freq[s]]
    zbuf[z] = total

    def send_sum(i):
        return pltpu.make_async_remote_copy(
            src_ref=zbuf.at[z], dst_ref=zbuf.at[z], send_sem=zs_sem.at[i], recv_sem=zr_sem.at[z],
            device_id={"pts": cols[i]}, device_id_type=MESH)

    def take_sum(i):
        other = cols[i] // 8
        return pltpu.make_async_remote_copy(
            src_ref=zbuf.at[z], dst_ref=zbuf.at[other], send_sem=zs_sem.at[i], recv_sem=zr_sem.at[other],
            device_id={"pts": cols[i]}, device_id_type=MESH)

    for i in range(3):
        send_sum(i).start()
    for i in (1, 2, 0):
        take_sum(i).wait_recv()
    gram = ((zbuf[0] + zbuf[1]) + (zbuf[2] + zbuf[3])) * (1.0 / 98304.0)

    turned = pltpu.roll(gram, 64, 1)
    upper = jnp.concatenate([jnp.where(low, gram, turned), jnp.where(low, turned, gram)], axis=0)
    flipped = jnp.concatenate([upper, upper], axis=0).T[:64]
    row = iota((64, 128), 0)
    col = iota((64, 128), 1) % 64
    real = jnp.where(col >= row, upper, flipped)
    imag = jnp.where(col < row, upper, jnp.where(col > row, -flipped, 0.0))
    full = jnp.concatenate([jnp.where(low, real, -imag), jnp.where(low, imag, real)], axis=0)
    r0, r1, r2 = split3(full)
    rmat[pl.ds(0, 128), pl.ds(0, 128)] = r0.astype(BF16)
    rmat[pl.ds(128, 128), pl.ds(0, 128)] = r1.astype(BF16)
    rmat[pl.ds(0, 128), pl.ds(128, 128)] = r2.astype(BF16)
    rmat[pl.ds(128, 128), pl.ds(128, 128)] = jnp.zeros((128, 128), BF16)

    diag = jnp.where((col == row) & low, upper, 0.0)
    trace = jnp.sum(jnp.sum(diag, axis=1, keepdims=True), axis=0, keepdims=True)
    tbuf[line] = jnp.broadcast_to(trace, (8, 128))

    def send_trace(i):
        return pltpu.make_async_remote_copy(
            src_ref=tbuf.at[line], dst_ref=tbuf.at[line], send_sem=ts_sem.at[i], recv_sem=tr_sem.at[line],
            device_id={"freq": lines[i]}, device_id_type=MESH)

    def take_trace(i):
        return pltpu.make_async_remote_copy(
            src_ref=tbuf.at[line], dst_ref=tbuf.at[lines[i]], send_sem=ts_sem.at[i], recv_sem=tr_sem.at[lines[i]],
            device_id={"freq": lines[i]}, device_id_type=MESH)

    for i in range(3):
        send_trace(i).start()

    def applied(vectors):
        pieces = []
        for v in vectors:
            pieces.extend(split3(v))
        while len(pieces) % 2:
            pieces.append(jnp.zeros((8, 128), F32))
        left = jnp.concatenate(pieces, axis=0).astype(BF16)
        out = jnp.dot(jnp.concatenate([left, left], axis=1), rmat[...], preferred_element_type=F32)
        results = []
        for i in range(len(vectors)):
            parts = [out[24 * i + 8 * k : 24 * i + 8 * k + 8] for k in range(3)]
            small = (parts[2][:, :128] + parts[0][:, 128:]) + (parts[1][:, 128:] + parts[2][:, 128:])
            results.append(parts[0][:, :128] + (parts[1][:, :128] + small))
        return results

    rank = iota((8, 128), 0)
    v = jnp.concatenate([basis[0, q], basis[1, q]], axis=1)
    iv = pltpu.roll(v, 64, 1) * -half
    for step in range(ITERS):
        zv, wv = applied([v, iv])
        scale = jnp.zeros((8, 128), F32)
        for j in range(8):
            zj = jnp.broadcast_to(zv[j : j + 1], (8, 128))
            wj = jnp.broadcast_to(wv[j : j + 1], (8, 128))
            dot_real = jnp.broadcast_to(jnp.sum(zj * zv, axis=1, keepdims=True), (8, 128))
            norm = jnp.broadcast_to(dot_real[j : j + 1], (8, 128))
            factor = lax.rsqrt(norm * (1.0 / 64) + 1e-06)
            scale = jnp.where(rank == j, factor, scale)
            if j < 7:
                dot_imag = jnp.broadcast_to(jnp.sum(wj * zv, axis=1, keepdims=True), (8, 128))
                inverse = jnp.where(rank > j, factor * factor * (1.0 / 64), 0.0)
                coef_real = dot_real * inverse
                coef_imag = dot_imag * inverse
                zv, wv = (
                    zv - (coef_real * zj + coef_imag * wj),
                    wv - (coef_real * wj - coef_imag * zj),
                )
        v = zv * scale
        iv = wv * scale
    vbuf[q] = v

    def send_basis(s):
        return pltpu.make_async_remote_copy(
            src_ref=vbuf.at[q], dst_ref=vbuf.at[q], send_sem=vs_sem.at[s], recv_sem=vr_sem.at[q],
            device_id={"pts": rows[s]}, device_id_type=MESH)

    def take_basis(s):
        return pltpu.make_async_remote_copy(
            src_ref=vbuf.at[q], dst_ref=vbuf.at[freq[s]], send_sem=vs_sem.at[s], recv_sem=vr_sem.at[freq[s]],
            device_id={"pts": rows[s]}, device_id_type=MESH)

    for s in range(7):
        send_basis(s).start()

    def send_aux(s):
        return pltpu.make_async_remote_copy(
            src_ref=abuf.at[q], dst_ref=abuf.at[q], send_sem=as_sem.at[s], recv_sem=ar_sem.at[q],
            device_id={"pts": rows[s]}, device_id_type=MESH)

    def take_aux(s):
        return pltpu.make_async_remote_copy(
            src_ref=abuf.at[q], dst_ref=abuf.at[freq[s]], send_sem=as_sem.at[s], recv_sem=ar_sem.at[freq[s]],
            device_id={"pts": rows[s]}, device_id_type=MESH)

    (zv,) = applied([v])
    rayleigh = jnp.sum(v * zv, axis=1, keepdims=True) * (1.0 / 64)
    spread = jnp.sum(jnp.where(rank == iota((8, 128), 1), rayleigh, 0.0), axis=0, keepdims=True)
    for i in (1, 2, 0):
        take_trace(i).wait_recv()
    group = (tbuf[0] + tbuf[1]) + (tbuf[2] + tbuf[3])
    abuf[q] = jnp.where(rank == 0, spread, group)
    for s in range(7):
        send_aux(s).start()

    undo = lax.rsqrt(w) * (1.0 / 64)

    def store(s, part):
        return pltpu.make_async_copy(obuf.at[s, part], modes_out.at[part, freq[s]], out_sem.at[s, part])

    for s in reversed(range(8)):
        if s < 7:
            take_basis(s).wait_recv()
        vec = vbuf[freq[s]]
        other = pltpu.roll(vec, 64, 1)
        basis_out[0, freq[s]] = vec[:, :64]
        basis_out[1, freq[s]] = other[:, :64]
        left = jnp.concatenate([vec * half, other], axis=0)
        left_hi = left.astype(BF16)
        left_lo = (left - left_hi.astype(F32)).astype(BF16)
        left = jnp.concatenate([left_hi, left_lo], axis=0)
        left = jnp.concatenate([left, left], axis=1)
        for c in range(3):
            out = jnp.dot(left, ybuf[s, :, pl.ds(c * 1024, 1024)], preferred_element_type=F32)
            out = (out[:16] + out[16:]) * undo
            obuf[s, 0, c] = out[:8]
            obuf[s, 1, c] = out[8:]
        store(s, 0).start()
        store(s, 1).start()

    for s in range(7):
        take_aux(s).wait_recv()
    total = jnp.zeros((1, 128), F32)
    for f in range(8):
        total = total + abuf[f, 1:2]
    for f in range(8):
        spec_out[pl.ds(f, 1), :] = (abuf[f, 0:1] * 2048.0 / total)[:, :8]

    for s in range(7):
        send_product(s).wait_send()
        send_basis(s).wait_send()
        send_aux(s).wait_send()
    for i in range(3):
        send_sum(i).wait_send()
        send_trace(i).wait_send()
    for s in range(8):
        store(s, 0).wait()
        store(s, 1).wait()


def per_device(data, quad_weight, basis):
    data = jnp.transpose(data, (0, 1, 3, 2, 4))
    basis = jnp.transpose(basis, (0, 1, 3, 2))
    vmem = pl.BlockSpec(memory_space=pltpu.VMEM)
    hbm = pl.BlockSpec(memory_space=pl.ANY)
    dma = pltpu.SemaphoreType.DMA
    basis_out, spectrum, modes = pl.pallas_call(
        kernel,
        out_shape=(
            jax.ShapeDtypeStruct((2, 8, 8, 64), F32),
            jax.ShapeDtypeStruct((8, 8), F32),
            jax.ShapeDtypeStruct((2, 8, 3, 8, 1024), F32),
        ),
        in_specs=[hbm, vmem, vmem],
        out_specs=(vmem, vmem, hbm),
        scratch_shapes=[
            pltpu.VMEM((8, 2, 3, 64, 1024), F32),
            pltpu.VMEM((8, 256, 3072), BF16),
            pltpu.VMEM((7, 32, 128), F32),
            pltpu.VMEM((8, 32, 128), F32),
            pltpu.VMEM((4, 32, 128), F32),
            pltpu.VMEM((4, 8, 128), F32),
            pltpu.VMEM((8, 8, 128), F32),
            pltpu.VMEM((8, 8, 128), F32),
            pltpu.VMEM((256, 256), BF16),
            pltpu.VMEM((8, 2, 3, 8, 1024), F32),
            dma((8, 2)), dma((8, 2)), dma((7,)), dma((8,)), dma((3,)), dma((4,)),
            dma((3,)), dma((4,)), dma((7,)), dma((8,)), dma((7,)), dma((8,)),
        ],
        compiler_params=pltpu.CompilerParams(
            collective_id=0, has_side_effects=True, vmem_limit_bytes=48 * 1024 * 1024
        ),
        name="spod",
    )(data, quad_weight.reshape(1, -1), basis)
    return (
        jnp.transpose(basis_out, (0, 1, 3, 2)),
        spectrum,
        jnp.transpose(modes, (0, 1, 3, 2, 4)),
    )


def solution(mesh):
    in_specs = (P(None, "freq", None, None, "pts"), P("pts"), P(None, "freq", None, None))
    out_specs = (P(None, "freq", None, None), P("freq", None), P(None, "freq", None, None, "pts"))
    return jax.shard_map(
        per_device, mesh=mesh, in_specs=in_specs, out_specs=out_specs, check_vma=False
    )
```

```python
import jax
import jax.numpy as jnp
from jax import lax
from jax.experimental import pallas as pl
from jax.experimental.pallas import tpu as pltpu
from jax.sharding import PartitionSpec as P

ITERS = 4
AHEAD = 8
FIRST = 2
HELLO = 3
F32 = jnp.float32
BF16 = jnp.bfloat16
MESH = pl.DeviceIdType.MESH


def split3(value):
    first = value.astype(BF16).astype(F32)
    rest = value - first
    second = rest.astype(BF16).astype(F32)
    return first, second, rest - second


def iota(shape, dim):
    return lax.broadcasted_iota(jnp.int32, shape, dim)


def order(own):
    x = own // 2
    core = own % 2
    sign = 1 - 2 * ((3 - x) // 3)
    near = [(2, 0), (2, 1), (sign, 0), (sign, 1), (-sign, 0), (-sign, 1), (0, 1), (0, 0)]
    return [((x + dx + 4) % 4) * 2 + (core + dc) % 2 for dx, dc in near]


def opening(data, out, sem):
    freq = order(lax.axis_index("pts") % 8)
    copies = [
        pltpu.make_async_copy(data.at[:, freq[s]], out.at[s], sem.at[s]) for s in range(FIRST)
    ]
    for copy in copies:
        copy.start()
    for copy in copies:
        copy.wait()


def kernel(
    data, weight, start, first, basis_out, spec_out, modes_out,
    wbuf, sbuf, xbuf, pbuf, rbuf, gbuf, tbuf, vbuf, abuf, rmat,
    in_sem, load_sem, ps_sem, pr_sem, gs_sem, ts_sem, tr_sem, vs_sem, vr_sem, as_sem, ar_sem, ready,
    *ybuf,
):
    me = lax.axis_index("pts")
    line = lax.axis_index("freq")
    z = me // 8
    own = me % 8
    x = own // 2
    core = own % 2
    freq = order(own)
    goal = z * 8
    top = z // 3
    everyone = [
        zt * 8 + ((x + dx) % 4) * 2 + (core + dc) % 2
        for zt in (0, 1, 2, 3) for dx in (2, 1, 3, 0) for dc in (1, 0)
    ][:31]
    lines = [(line + d) % 4 for d in (2, 1, 3)]

    def load(s):
        return pltpu.make_async_copy(data.at[:, freq[s]], xbuf.at[s - FIRST], load_sem.at[s])

    get_weight = pltpu.make_async_copy(weight, wbuf, in_sem.at[0])
    get_start = pltpu.make_async_copy(start.at[:, own], sbuf, in_sem.at[1])
    get_weight.start()
    for s in range(FIRST, 8):
        load(s).start()
    get_start.start()

    barrier = pltpu.get_barrier_semaphore()

    def greet(peer):
        pl.semaphore_signal(barrier, inc=1, device_id={"pts": peer}, device_id_type=MESH)

    for s in range(7):
        greet(z * 8 + freq[s])

    @pl.when(z < 3)
    def _():
        for f in range(8):
            greet(24 + f)

    @pl.when(z == 3)
    def _():
        for peer in lines:
            pl.semaphore_signal(barrier, inc=1, device_id={"freq": peer}, device_id_type=MESH)

    get_weight.wait()
    w = wbuf[...]
    root = jnp.sqrt(w)
    low = iota((1, 128), 1) < 64
    half = jnp.where(low, 1.0, -1.0).astype(F32)

    def split(s, hook):
        if s >= FIRST:
            load(s).wait()
        for c in range(3):
            if c == 1:
                hook()
            span = pl.ds(c * 1024, 1024)
            for part in range(2):
                for r in range(0, 64, 16):
                    y = (first[s, part, c, pl.ds(r, 16)] if s < FIRST else xbuf[s - FIRST, part, c, pl.ds(r, 16)]) * root
                    hi = y.astype(BF16)
                    lo = (y - hi.astype(F32)).astype(BF16)
                    ybuf[s][pl.ds(part * 64 + r, 16), span] = hi
                    ybuf[s][pl.ds(128 + part * 64 + r, 16), span] = lo

    def product(s):
        total = None
        for k in range(2):
            both = ybuf[s][:, pl.ds(k * 1536, 1536)]
            m = lax.dot_general(both, both, (((1,), (1,)), ((), ())), preferred_element_type=F32)
            m = (m[:128, :128] + m[128:, 128:]) + (m[:128, 128:] + m[128:, :128])
            total = m if total is None else total + m
        return total

    def packed(m):
        top, bottom = m[:64], m[64:]
        straight = top + half * pltpu.roll(bottom, 64, 1)
        swapped = pltpu.roll(top, 64, 1) - half * bottom
        row = iota((64, 128), 0)
        col = iota((64, 128), 1) % 64
        upper = jnp.where(low == (col >= row), straight, swapped)
        return jnp.where(low, upper[:32], upper[32:])

    def send_product(s):
        return pltpu.make_async_remote_copy(
            src_ref=pbuf.at[s], dst_ref=rbuf.at[own], send_sem=ps_sem.at[s], recv_sem=pr_sem.at[own],
            device_id={"pts": goal + freq[s]}, device_id_type=MESH)

    def take_product(at):
        return pltpu.make_async_remote_copy(
            src_ref=pbuf.at[0], dst_ref=rbuf.at[at], send_sem=ps_sem.at[0], recv_sem=pr_sem.at[at],
            device_id={"pts": goal + freq[0]}, device_id_type=MESH)

    def send_row():
        return pltpu.make_async_remote_copy(
            src_ref=gbuf, dst_ref=rbuf.at[8 + z], send_sem=gs_sem.at[0], recv_sem=pr_sem.at[8 + z],
            device_id={"pts": 24 + own}, device_id_type=MESH)

    before = None

    def passed(s):
        if not s:
            return
        pbuf[s - 1] = packed(before)
        if s == HELLO:
            pl.semaphore_wait(barrier, 7 + 27 * top)

            @pl.when(z == 3)
            def _():
                for peer in (0, 8, 16):
                    pl.semaphore_signal(
                        ready, inc=1, device_id={"pts": peer + own}, device_id_type=MESH)
        for k in range(s) if s == HELLO else [s - 1] if s > HELLO else []:
            send_product(k).start()

    for s in range(8):
        split(s, lambda: passed(s))
        before = product(s)
    pbuf[7] = packed(before)

    def send_trace(i):
        return pltpu.make_async_remote_copy(
            src_ref=tbuf.at[line], dst_ref=tbuf.at[line], send_sem=ts_sem.at[i], recv_sem=tr_sem.at[line],
            device_id={"freq": lines[i]}, device_id_type=MESH)

    def take_trace(i):
        return pltpu.make_async_remote_copy(
            src_ref=tbuf.at[line], dst_ref=tbuf.at[lines[i]], send_sem=ts_sem.at[i], recv_sem=tr_sem.at[lines[i]],
            device_id={"freq": lines[i]}, device_id_type=MESH)

    def send_basis(i):
        return pltpu.make_async_remote_copy(
            src_ref=vbuf.at[own], dst_ref=vbuf.at[own], send_sem=vs_sem.at[i], recv_sem=vr_sem.at[own],
            device_id={"pts": everyone[i]}, device_id_type=MESH)

    def take_basis(s):
        return pltpu.make_async_remote_copy(
            src_ref=vbuf.at[own], dst_ref=vbuf.at[freq[s]], send_sem=vs_sem.at[0], recv_sem=vr_sem.at[freq[s]],
            device_id={"pts": 24 + freq[s]}, device_id_type=MESH)

    def send_aux(i):
        return pltpu.make_async_remote_copy(
            src_ref=abuf.at[own], dst_ref=abuf.at[own], send_sem=as_sem.at[i], recv_sem=ar_sem.at[own],
            device_id={"pts": everyone[i]}, device_id_type=MESH)

    def take_aux(s):
        return pltpu.make_async_remote_copy(
            src_ref=abuf.at[own], dst_ref=abuf.at[freq[s]], send_sem=as_sem.at[0], recv_sem=ar_sem.at[freq[s]],
            device_id={"pts": 24 + freq[s]}, device_id_type=MESH)

    def applied(vectors):
        pieces = []
        for v in vectors:
            pieces.extend(split3(v))
        while len(pieces) % 2:
            pieces.append(jnp.zeros((8, 128), F32))
        left = jnp.concatenate(pieces, axis=0).astype(BF16)
        out = jnp.dot(jnp.concatenate([left, left], axis=1), rmat[...], preferred_element_type=F32)
        results = []
        for i in range(len(vectors)):
            parts = [out[24 * i + 8 * k : 24 * i + 8 * k + 8] for k in range(3)]
            small = (parts[2][:, :128] + parts[0][:, 128:]) + (parts[1][:, 128:] + parts[2][:, 128:])
            results.append(parts[0][:, :128] + (parts[1][:, :128] + small))
        return results

    get_start.wait()

    @pl.when(z < 3)
    def _():
        total = pbuf[7]
        for s in range(7):
            take_product(freq[s]).wait_recv()
            total = total + rbuf[freq[s]]
        gbuf[...] = total
        pl.semaphore_wait(ready, 1)
        send_row().start()
        send_row().wait_send()

    @pl.when(z == 3)
    def _():
        total = pbuf[7]
        for s in range(7):
            take_product(freq[s]).wait_recv()
            total = total + rbuf[freq[s]]
        for at in (8, 9, 10):
            take_product(at).wait_recv()
            total = total + rbuf[at]
        gram = total * (1.0 / 98304.0)
        turned = pltpu.roll(gram, 64, 1)
        upper = jnp.concatenate([jnp.where(low, gram, turned), jnp.where(low, turned, gram)], axis=0)
        flipped = jnp.concatenate([upper, upper], axis=0).T[:64]
        row = iota((64, 128), 0)
        col = iota((64, 128), 1) % 64
        real = jnp.where(col >= row, upper, flipped)
        imag = jnp.where(col < row, upper, jnp.where(col > row, -flipped, 0.0))
        full = jnp.concatenate([jnp.where(low, real, -imag), jnp.where(low, imag, real)], axis=0)
        r0, r1, r2 = split3(full)
        rmat[pl.ds(0, 128), pl.ds(0, 128)] = r0.astype(BF16)
        rmat[pl.ds(128, 128), pl.ds(0, 128)] = r1.astype(BF16)
        rmat[pl.ds(0, 128), pl.ds(128, 128)] = r2.astype(BF16)
        rmat[pl.ds(128, 128), pl.ds(128, 128)] = jnp.zeros((128, 128), BF16)

        diag = jnp.where((col == row) & low, upper, 0.0)
        trace = jnp.sum(jnp.sum(diag, axis=1, keepdims=True), axis=0, keepdims=True)
        tbuf[line] = jnp.broadcast_to(trace, (8, 128))
        for i in range(3):
            send_trace(i).start()

        rank = iota((8, 128), 0)
        v = jnp.concatenate([sbuf[0], sbuf[1]], axis=1)
        iv = pltpu.roll(v, 64, 1) * -half
        for step in range(ITERS):
            zv, wv = applied([v, iv])
            scale = jnp.zeros((8, 128), F32)
            for j in range(8):
                zj = jnp.broadcast_to(zv[j : j + 1], (8, 128))
                wj = jnp.broadcast_to(wv[j : j + 1], (8, 128))
                dot_real = jnp.broadcast_to(jnp.sum(zj * zv, axis=1, keepdims=True), (8, 128))
                norm = jnp.broadcast_to(dot_real[j : j + 1], (8, 128))
                factor = lax.rsqrt(norm * (1.0 / 64) + 1e-06)
                scale = jnp.where(rank == j, factor, scale)
                if j < 7:
                    dot_imag = jnp.broadcast_to(jnp.sum(wj * zv, axis=1, keepdims=True), (8, 128))
                    inverse = jnp.where(rank > j, factor * factor * (1.0 / 64), 0.0)
                    coef_real = dot_real * inverse
                    coef_imag = dot_imag * inverse
                    zv, wv = (
                        zv - (coef_real * zj + coef_imag * wj),
                        wv - (coef_real * wj - coef_imag * zj),
                    )
            v = zv * scale
            iv = wv * scale
        vbuf[own] = v
        for i in range(31):
            send_basis(i).start()

        (zv,) = applied([v])
        rayleigh = jnp.sum(v * zv, axis=1, keepdims=True) * (1.0 / 64)
        spread = jnp.sum(jnp.where(rank == iota((8, 128), 1), rayleigh, 0.0), axis=0, keepdims=True)
        for i in (1, 2, 0):
            take_trace(i).wait_recv()
        group = (tbuf[0] + tbuf[1]) + (tbuf[2] + tbuf[3])
        abuf[own] = jnp.where(rank == 0, spread, group)
        for i in range(31):
            send_aux(i).start()
        for i in range(3):
            send_trace(i).wait_send()

    undo = lax.rsqrt(w) * (1.0 / 64)

    for s in reversed(range(8)):
        if s < 7:
            take_basis(s).wait_recv()
        else:
            @pl.when(z < 3)
            def _():
                take_basis(7).wait_recv()
        vec = vbuf[freq[s]]
        other = pltpu.roll(vec, 64, 1)
        basis_out[0, freq[s]] = vec[:, :64]
        basis_out[1, freq[s]] = other[:, :64]
        left = jnp.concatenate([vec * half, other], axis=0)
        left_hi = left.astype(BF16)
        left_lo = (left - left_hi.astype(F32)).astype(BF16)
        left = jnp.concatenate([left_hi, left_lo], axis=0)
        left = jnp.concatenate([left, left], axis=1)
        for k in range(6):
            c, at = k // 2, k % 2 * 512
            out = jnp.dot(left, ybuf[s][:, pl.ds(k * 512, 512)], preferred_element_type=F32)
            out = (out[:16] + out[16:]) * undo[:, at : at + 512]
            modes_out[0, freq[s], c, :, pl.ds(at, 512)] = out[:8]
            modes_out[1, freq[s], c, :, pl.ds(at, 512)] = out[8:]

    for s in range(7):
        take_aux(s).wait_recv()

    @pl.when(z < 3)
    def _():
        take_aux(7).wait_recv()

    total = jnp.zeros((1, 128), F32)
    for f in range(8):
        total = total + abuf[f, 1:2]
    for f in range(8):
        spec_out[pl.ds(f, 1), :] = (abuf[f, 0:1] * 2048.0 / total)[:, :8]

    for s in range(7):
        send_product(s).wait_send()

    @pl.when(z == 3)
    def _():
        for i in range(31):
            send_basis(i).wait_send()
            send_aux(i).wait_send()


def writer(basis_in, spec_in, modes_in, basis_out, spec_out, modes_out, sem):
    copies = [
        pltpu.make_async_copy(modes_in, modes_out, sem.at[0]),
        pltpu.make_async_copy(basis_in, basis_out, sem.at[1]),
        pltpu.make_async_copy(spec_in, spec_out, sem.at[2]),
    ]
    for copy in copies:
        copy.start()
    for copy in copies:
        copy.wait()


def per_device(data, quad_weight, basis):
    data = jnp.transpose(data, (0, 1, 3, 2, 4))
    basis = jnp.transpose(basis, (0, 1, 3, 2))
    vmem = pl.BlockSpec(memory_space=pltpu.VMEM)
    hbm = pl.BlockSpec(memory_space=pltpu.HBM)
    dma = pltpu.SemaphoreType.DMA
    shapes = (
        jax.ShapeDtypeStruct((2, 8, 8, 64), F32),
        jax.ShapeDtypeStruct((8, 8), F32),
        jax.ShapeDtypeStruct((2, 8, 3, 8, 1024), F32),
    )
    first = pl.pallas_call(
        opening,
        out_shape=jax.ShapeDtypeStruct((FIRST, 2, 3, 64, 1024), F32),
        in_specs=[hbm],
        out_specs=vmem,
        scratch_shapes=[dma((FIRST,))],
        compiler_params=pltpu.CompilerParams(vmem_limit_bytes=48 * 1024 * 1024),
        cost_estimate=pl.CostEstimate(flops=10**9, bytes_accessed=6 * 10**6, transcendentals=0),
        name="opening",
    )(data)
    results = pl.pallas_call(
        kernel,
        out_shape=shapes,
        in_specs=[hbm, hbm, hbm, vmem],
        out_specs=(vmem, vmem, vmem),
        scratch_shapes=[
            pltpu.VMEM((1, 1024), F32),
            pltpu.VMEM((2, 8, 64), F32),
            pltpu.VMEM((8 - FIRST, 2, 3, 64, 1024), F32),
            pltpu.VMEM((8, 32, 128), F32),
            pltpu.VMEM((11, 32, 128), F32),
            pltpu.VMEM((32, 128), F32),
            pltpu.VMEM((4, 8, 128), F32),
            pltpu.VMEM((8, 8, 128), F32),
            pltpu.VMEM((8, 8, 128), F32),
            pltpu.VMEM((256, 256), BF16),
            dma((2,)), dma((8,)), dma((8,)), dma((11,)), dma((1,)),
            dma((3,)), dma((4,)), dma((31,)), dma((8,)), dma((31,)), dma((8,)),
            pltpu.SemaphoreType.REGULAR,
            *[pltpu.VMEM((256, 3072), BF16) for _ in range(8)],
        ],
        compiler_params=pltpu.CompilerParams(
            collective_id=0, has_side_effects=True, vmem_limit_bytes=48 * 1024 * 1024
        ),
        name="spod",
    )(data, quad_weight.reshape(1, -1), basis, first)
    basis_out, spectrum, modes = pl.pallas_call(
        writer,
        out_shape=shapes,
        in_specs=[vmem, vmem, vmem],
        out_specs=(hbm, hbm, hbm),
        scratch_shapes=[dma((3,))],
        compiler_params=pltpu.CompilerParams(vmem_limit_bytes=4 * 1024 * 1024),
        name="writer",
    )(*results)
    return (
        jnp.transpose(basis_out, (0, 1, 3, 2)),
        spectrum,
        jnp.transpose(modes, (0, 1, 3, 2, 4)),
    )


def solution(mesh):
    in_specs = (P(None, "freq", None, None, "pts"), P("pts"), P(None, "freq", None, None))
    out_specs = (P(None, "freq", None, None), P("freq", None), P(None, "freq", None, None, "pts"))
    return jax.shard_map(
        per_device, mesh=mesh, in_specs=in_specs, out_specs=out_specs, check_vma=False
    )
```

```python
import jax
import jax.numpy as jnp
from jax import lax
from jax.experimental import pallas as pl
from jax.experimental.pallas import tpu as pltpu
from jax.sharding import PartitionSpec as P

ITERS = 4
AHEAD = 8
FIRST = 2
HELLO = 3
F32 = jnp.float32
BF16 = jnp.bfloat16
MESH = pl.DeviceIdType.MESH


def split3(value):
    first = value.astype(BF16).astype(F32)
    rest = value - first
    second = rest.astype(BF16).astype(F32)
    return first, second, rest - second


def iota(shape, dim):
    return lax.broadcasted_iota(jnp.int32, shape, dim)


def order(own):
    x = own // 2
    core = own % 2
    sign = 1 - 2 * ((3 - x) // 3)
    near = [(2, 0), (2, 1), (sign, 0), (sign, 1), (-sign, 0), (-sign, 1), (0, 1), (0, 0)]
    return [((x + dx + 4) % 4) * 2 + (core + dc) % 2 for dx, dc in near]


def opening(data, out, sem):
    freq = order(lax.axis_index("pts") % 8)
    copies = [
        pltpu.make_async_copy(data.at[:, freq[s]], out.at[s], sem.at[s]) for s in range(FIRST)
    ]
    for copy in copies:
        copy.start()
    for copy in copies:
        copy.wait()


def kernel(
    data, weight, start, first, basis_out, spec_out, modes_out,
    xbuf, pbuf, rbuf, gbuf, tbuf, vbuf, abuf, rmat,
    load_sem, ps_sem, pr_sem, gs_sem, ts_sem, tr_sem, vs_sem, vr_sem, as_sem, ar_sem, ready,
    *ybuf,
):
    me = lax.axis_index("pts")
    line = lax.axis_index("freq")
    z = me // 8
    own = me % 8
    x = own // 2
    core = own % 2
    freq = order(own)
    goal = z * 8
    top = z // 3
    everyone = list(range(24)) + [
        24 + ((x + dx) % 4) * 2 + (core + dc) % 2 for dx in (2, 1, 3, 0) for dc in (1, 0)
    ][:7]
    lines = [(line + d) % 4 for d in (2, 1, 3)]

    def load(s):
        return pltpu.make_async_copy(data.at[:, freq[s]], xbuf.at[s - FIRST], load_sem.at[s])

    for s in range(FIRST, 8):
        load(s).start()

    barrier = pltpu.get_barrier_semaphore()

    def greet(peer):
        pl.semaphore_signal(barrier, inc=1, device_id={"pts": peer}, device_id_type=MESH)

    for s in range(7):
        greet(z * 8 + freq[s])

    @pl.when(z < 3)
    def _():
        for f in range(8):
            greet(24 + f)

    @pl.when(z == 3)
    def _():
        for peer in lines:
            pl.semaphore_signal(barrier, inc=1, device_id={"freq": peer}, device_id_type=MESH)

    w = weight[...]
    root = jnp.sqrt(w)
    low = iota((1, 128), 1) < 64
    half = jnp.where(low, 1.0, -1.0).astype(F32)

    def split(s, hook):
        if s >= FIRST:
            load(s).wait()
        for c in range(3):
            if c == 1:
                hook()
            span = pl.ds(c * 1024, 1024)
            for part in range(2):
                for r in range(0, 64, 16):
                    y = (first[s, part, c, pl.ds(r, 16)] if s < FIRST else xbuf[s - FIRST, part, c, pl.ds(r, 16)]) * root
                    hi = y.astype(BF16)
                    lo = (y - hi.astype(F32)).astype(BF16)
                    ybuf[s][pl.ds(part * 64 + r, 16), span] = hi
                    ybuf[s][pl.ds(128 + part * 64 + r, 16), span] = lo

    def product(s):
        total = None
        for k in range(2):
            both = ybuf[s][:, pl.ds(k * 1536, 1536)]
            m = lax.dot_general(both, both, (((1,), (1,)), ((), ())), preferred_element_type=F32)
            m = (m[:128, :128] + m[128:, 128:]) + (m[:128, 128:] + m[128:, :128])
            total = m if total is None else total + m
        return total

    def packed(m):
        top, bottom = m[:64], m[64:]
        straight = top + half * pltpu.roll(bottom, 64, 1)
        swapped = pltpu.roll(top, 64, 1) - half * bottom
        row = iota((64, 128), 0)
        col = iota((64, 128), 1) % 64
        upper = jnp.where(low == (col >= row), straight, swapped)
        return jnp.where(low, upper[:32], upper[32:])

    def send_product(s):
        return pltpu.make_async_remote_copy(
            src_ref=pbuf.at[s], dst_ref=rbuf.at[own], send_sem=ps_sem.at[s], recv_sem=pr_sem.at[own],
            device_id={"pts": goal + freq[s]}, device_id_type=MESH)

    def take_product(at):
        return pltpu.make_async_remote_copy(
            src_ref=pbuf.at[0], dst_ref=rbuf.at[at], send_sem=ps_sem.at[0], recv_sem=pr_sem.at[at],
            device_id={"pts": goal + freq[0]}, device_id_type=MESH)

    def send_row():
        return pltpu.make_async_remote_copy(
            src_ref=gbuf, dst_ref=rbuf.at[8 + z], send_sem=gs_sem.at[0], recv_sem=pr_sem.at[8 + z],
            device_id={"pts": 24 + own}, device_id_type=MESH)

    before = None

    def passed(s):
        if not s:
            return
        pbuf[s - 1] = packed(before)
        if s == HELLO:
            pl.semaphore_wait(barrier, 7 + 27 * top)

            @pl.when(z == 3)
            def _():
                for peer in (0, 8, 16):
                    pl.semaphore_signal(
                        ready, inc=1, device_id={"pts": peer + own}, device_id_type=MESH)
        for k in range(s) if s == HELLO else [s - 1] if s > HELLO else []:
            send_product(k).start()

    for s in range(8):
        split(s, lambda: passed(s))
        before = product(s)
    pbuf[7] = packed(before)

    def send_trace(i):
        return pltpu.make_async_remote_copy(
            src_ref=tbuf.at[line], dst_ref=tbuf.at[line], send_sem=ts_sem.at[i], recv_sem=tr_sem.at[line],
            device_id={"freq": lines[i]}, device_id_type=MESH)

    def take_trace(i):
        return pltpu.make_async_remote_copy(
            src_ref=tbuf.at[line], dst_ref=tbuf.at[lines[i]], send_sem=ts_sem.at[i], recv_sem=tr_sem.at[lines[i]],
            device_id={"freq": lines[i]}, device_id_type=MESH)

    def send_basis(i):
        return pltpu.make_async_remote_copy(
            src_ref=vbuf.at[own], dst_ref=vbuf.at[own], send_sem=vs_sem.at[i], recv_sem=vr_sem.at[own],
            device_id={"pts": everyone[i]}, device_id_type=MESH)

    def take_basis(s):
        return pltpu.make_async_remote_copy(
            src_ref=vbuf.at[own], dst_ref=vbuf.at[freq[s]], send_sem=vs_sem.at[0], recv_sem=vr_sem.at[freq[s]],
            device_id={"pts": 24 + freq[s]}, device_id_type=MESH)

    def send_aux(i):
        return pltpu.make_async_remote_copy(
            src_ref=abuf.at[own], dst_ref=abuf.at[own], send_sem=as_sem.at[i], recv_sem=ar_sem.at[own],
            device_id={"pts": everyone[i]}, device_id_type=MESH)

    def take_aux(s):
        return pltpu.make_async_remote_copy(
            src_ref=abuf.at[own], dst_ref=abuf.at[freq[s]], send_sem=as_sem.at[0], recv_sem=ar_sem.at[freq[s]],
            device_id={"pts": 24 + freq[s]}, device_id_type=MESH)

    def applied(vectors):
        pieces = []
        for v in vectors:
            pieces.extend(split3(v))
        while len(pieces) % 2:
            pieces.append(jnp.zeros((8, 128), F32))
        left = jnp.concatenate(pieces, axis=0).astype(BF16)
        out = jnp.dot(jnp.concatenate([left, left], axis=1), rmat[...], preferred_element_type=F32)
        results = []
        for i in range(len(vectors)):
            parts = [out[24 * i + 8 * k : 24 * i + 8 * k + 8] for k in range(3)]
            small = (parts[2][:, :128] + parts[0][:, 128:]) + (parts[1][:, 128:] + parts[2][:, 128:])
            results.append(parts[0][:, :128] + (parts[1][:, :128] + small))
        return results


    @pl.when(z < 3)
    def _():
        total = pbuf[7]
        for s in range(7):
            take_product(freq[s]).wait_recv()
            total = total + rbuf[freq[s]]
        gbuf[...] = total
        pl.semaphore_wait(ready, 1)
        send_row().start()
        send_row().wait_send()

    @pl.when(z == 3)
    def _():
        total = pbuf[7]
        for s in range(7):
            take_product(freq[s]).wait_recv()
            total = total + rbuf[freq[s]]
        for at in (8, 9, 10):
            take_product(at).wait_recv()
            total = total + rbuf[at]
        gram = total * (1.0 / 98304.0)
        turned = pltpu.roll(gram, 64, 1)
        upper = jnp.concatenate([jnp.where(low, gram, turned), jnp.where(low, turned, gram)], axis=0)
        flipped = jnp.concatenate([upper, upper], axis=0).T[:64]
        row = iota((64, 128), 0)
        col = iota((64, 128), 1) % 64
        real = jnp.where(col >= row, upper, flipped)
        imag = jnp.where(col < row, upper, jnp.where(col > row, -flipped, 0.0))
        full = jnp.concatenate([jnp.where(low, real, -imag), jnp.where(low, imag, real)], axis=0)
        r0, r1, r2 = split3(full)
        rmat[pl.ds(0, 128), pl.ds(0, 128)] = r0.astype(BF16)
        rmat[pl.ds(128, 128), pl.ds(0, 128)] = r1.astype(BF16)
        rmat[pl.ds(0, 128), pl.ds(128, 128)] = r2.astype(BF16)
        rmat[pl.ds(128, 128), pl.ds(128, 128)] = jnp.zeros((128, 128), BF16)

        diag = jnp.where((col == row) & low, upper, 0.0)
        trace = jnp.sum(jnp.sum(diag, axis=1, keepdims=True), axis=0, keepdims=True)
        tbuf[line] = jnp.broadcast_to(trace, (8, 128))
        for i in range(3):
            send_trace(i).start()

        rank = iota((8, 128), 0)
        v = jnp.concatenate([start[0, own], start[1, own]], axis=1)
        iv = pltpu.roll(v, 64, 1) * -half
        scale = None
        zv, wv = v, iv
        for step in range(ITERS):
            zv, wv = applied([zv, wv])
            if scale is not None:
                zv, wv = zv * scale, wv * scale
            scale = jnp.zeros((8, 128), F32)
            for j in range(8):
                zj = jnp.broadcast_to(zv[j : j + 1], (8, 128))
                wj = jnp.broadcast_to(wv[j : j + 1], (8, 128))
                dot_real = jnp.broadcast_to(jnp.sum(zj * zv, axis=1, keepdims=True), (8, 128))
                norm = jnp.broadcast_to(dot_real[j : j + 1], (8, 128))
                factor = lax.rsqrt(norm * (1.0 / 64) + 1e-06)
                scale = jnp.where(rank == j, factor, scale)
                if j < 7:
                    dot_imag = jnp.broadcast_to(jnp.sum(wj * zv, axis=1, keepdims=True), (8, 128))
                    inverse = jnp.where(rank > j, factor * factor * (1.0 / 64), 0.0)
                    coef_real = dot_real * inverse
                    coef_imag = dot_imag * inverse
                    zv, wv = (
                        zv - (coef_real * zj + coef_imag * wj),
                        wv - (coef_real * wj - coef_imag * zj),
                    )
        v = zv * scale
        vbuf[own] = v
        for i in range(31):
            send_basis(i).start()

        (zv,) = applied([v])
        rayleigh = jnp.sum(v * zv, axis=1, keepdims=True) * (1.0 / 64)
        spread = jnp.sum(jnp.where(rank == iota((8, 128), 1), rayleigh, 0.0), axis=0, keepdims=True)
        for i in (1, 2, 0):
            take_trace(i).wait_recv()
        group = (tbuf[0] + tbuf[1]) + (tbuf[2] + tbuf[3])
        abuf[own] = jnp.where(low, spread, group[:1])
        for i in range(31):
            send_aux(i).start()
        for i in range(3):
            send_trace(i).wait_send()

    undo = lax.rsqrt(w) * (1.0 / 64)

    for s in reversed(range(8)):
        if s < 7:
            take_basis(s).wait_recv()
        else:
            @pl.when(z < 3)
            def _():
                take_basis(7).wait_recv()
        vec = vbuf[freq[s]]
        other = pltpu.roll(vec, 64, 1)
        basis_out[0, freq[s]] = vec[:, :64]
        basis_out[1, freq[s]] = other[:, :64]
        left = jnp.concatenate([vec * half, other], axis=0)
        left_hi = left.astype(BF16)
        left_lo = (left - left_hi.astype(F32)).astype(BF16)
        left = jnp.concatenate([left_hi, left_lo], axis=0)
        left = jnp.concatenate([left, left], axis=1)
        for k in range(6):
            c, at = k // 2, k % 2 * 512
            out = jnp.dot(left, ybuf[s][:, pl.ds(k * 512, 512)], preferred_element_type=F32)
            out = (out[:16] + out[16:]) * undo[:, at : at + 512]
            modes_out[0, freq[s], c, :, pl.ds(at, 512)] = out[:8]
            modes_out[1, freq[s], c, :, pl.ds(at, 512)] = out[8:]

    for s in range(7):
        take_aux(s).wait_recv()

    @pl.when(z < 3)
    def _():
        take_aux(7).wait_recv()

    total = jnp.zeros((1, 8), F32)
    for f in range(8):
        total = total + abuf[f, :, 64:72]
    for f in range(8):
        spec_out[pl.ds(f, 1), :] = abuf[f, :, :8] * 2048.0 / total

    for s in range(7):
        send_product(s).wait_send()

    @pl.when(z == 3)
    def _():
        for i in range(31):
            send_basis(i).wait_send()
            send_aux(i).wait_send()


def writer(basis_in, spec_in, modes_in, basis_out, spec_out, modes_out, sem):
    copies = [
        pltpu.make_async_copy(modes_in, modes_out, sem.at[0]),
        pltpu.make_async_copy(basis_in, basis_out, sem.at[1]),
        pltpu.make_async_copy(spec_in, spec_out, sem.at[2]),
    ]
    for copy in copies:
        copy.start()
    for copy in copies:
        copy.wait()


def per_device(data, quad_weight, basis):
    data = jnp.transpose(data, (0, 1, 3, 2, 4))
    basis = jnp.transpose(basis, (0, 1, 3, 2))
    vmem = pl.BlockSpec(memory_space=pltpu.VMEM)
    hbm = pl.BlockSpec(memory_space=pltpu.HBM)
    dma = pltpu.SemaphoreType.DMA
    shapes = (
        jax.ShapeDtypeStruct((2, 8, 8, 64), F32),
        jax.ShapeDtypeStruct((8, 8), F32),
        jax.ShapeDtypeStruct((2, 8, 3, 8, 1024), F32),
    )
    first = pl.pallas_call(
        opening,
        out_shape=jax.ShapeDtypeStruct((FIRST, 2, 3, 64, 1024), F32),
        in_specs=[hbm],
        out_specs=vmem,
        scratch_shapes=[dma((FIRST,))],
        compiler_params=pltpu.CompilerParams(vmem_limit_bytes=48 * 1024 * 1024),
        cost_estimate=pl.CostEstimate(flops=10**9, bytes_accessed=6 * 10**6, transcendentals=0),
        name="opening",
    )(data)
    results = pl.pallas_call(
        kernel,
        out_shape=shapes,
        in_specs=[hbm, vmem, vmem, vmem],
        out_specs=(vmem, vmem, vmem),
        scratch_shapes=[
            pltpu.VMEM((8 - FIRST, 2, 3, 64, 1024), F32),
            pltpu.VMEM((8, 32, 128), F32),
            pltpu.VMEM((11, 32, 128), F32),
            pltpu.VMEM((32, 128), F32),
            pltpu.VMEM((4, 8, 128), F32),
            pltpu.VMEM((8, 8, 128), F32),
            pltpu.VMEM((8, 1, 128), F32),
            pltpu.VMEM((256, 256), BF16),
            dma((8,)), dma((8,)), dma((11,)), dma((1,)),
            dma((3,)), dma((4,)), dma((31,)), dma((8,)), dma((31,)), dma((8,)),
            pltpu.SemaphoreType.REGULAR,
            *[pltpu.VMEM((256, 3072), BF16) for _ in range(8)],
        ],
        compiler_params=pltpu.CompilerParams(
            collective_id=0, has_side_effects=True, vmem_limit_bytes=48 * 1024 * 1024
        ),
        name="spod",
    )(data, quad_weight.reshape(1, -1), basis, first)
    basis_out, spectrum, modes = pl.pallas_call(
        writer,
        out_shape=shapes,
        in_specs=[vmem, vmem, vmem],
        out_specs=(hbm, hbm, hbm),
        scratch_shapes=[dma((3,))],
        compiler_params=pltpu.CompilerParams(vmem_limit_bytes=4 * 1024 * 1024),
        name="writer",
    )(*results)
    return (
        jnp.transpose(basis_out, (0, 1, 3, 2)),
        spectrum,
        jnp.transpose(modes, (0, 1, 3, 2, 4)),
    )


def solution(mesh):
    in_specs = (P(None, "freq", None, None, "pts"), P("pts"), P(None, "freq", None, None))
    out_specs = (P(None, "freq", None, None), P("freq", None), P(None, "freq", None, None, "pts"))
    return jax.shard_map(
        per_device, mesh=mesh, in_specs=in_specs, out_specs=out_specs, check_vma=False
    )
```

```python
import jax
import jax.numpy as jnp
from jax import lax
from jax.experimental import pallas as pl
from jax.experimental.pallas import tpu as pltpu
from jax.sharding import PartitionSpec as P

ITERS = 4
AHEAD = 8
FIRST = 2
HELLO = 3
F32 = jnp.float32
BF16 = jnp.bfloat16
MESH = pl.DeviceIdType.MESH


def split3(value):
    first = value.astype(BF16).astype(F32)
    rest = value - first
    second = rest.astype(BF16).astype(F32)
    return first, second, rest - second


def iota(shape, dim):
    return lax.broadcasted_iota(jnp.int32, shape, dim)


def order(own):
    x = own // 2
    core = own % 2
    sign = 1 - 2 * ((3 - x) // 3)
    near = [(2, 0), (2, 1), (sign, 0), (sign, 1), (-sign, 0), (-sign, 1), (0, 1), (0, 0)]
    return [((x + dx + 4) % 4) * 2 + (core + dc) % 2 for dx, dc in near]


def opening(data, out, sem):
    freq = order(lax.axis_index("pts") % 8)
    copies = [
        pltpu.make_async_copy(data.at[:, freq[s]], out.at[s], sem.at[s]) for s in range(FIRST)
    ]
    for copy in copies:
        copy.start()
    for copy in copies:
        copy.wait()


def kernel(
    data, weight, start, first, basis_out, spec_out, modes_out,
    xbuf, pbuf, rbuf, gbuf, tbuf, vbuf, abuf, rmat,
    load_sem, ps_sem, pr_sem, gs_sem, ts_sem, tr_sem, vs_sem, vr_sem, as_sem, ar_sem, ready,
    *ybuf,
):
    me = lax.axis_index("pts")
    line = lax.axis_index("freq")
    z = me // 8
    own = me % 8
    x = own // 2
    core = own % 2
    freq = order(own)
    goal = z * 8
    top = z // 3
    everyone = list(range(24)) + [
        24 + ((x + dx) % 4) * 2 + (core + dc) % 2 for dx in (2, 1, 3, 0) for dc in (1, 0)
    ][:7]
    lines = [(line + d) % 4 for d in (2, 1, 3)]

    def load(s):
        return pltpu.make_async_copy(data.at[:, freq[s]], xbuf.at[s - FIRST], load_sem.at[s])

    for s in range(FIRST, 8):
        load(s).start()

    barrier = pltpu.get_barrier_semaphore()

    def greet(peer):
        pl.semaphore_signal(barrier, inc=1, device_id={"pts": peer}, device_id_type=MESH)

    for s in range(7):
        greet(z * 8 + freq[s])

    @pl.when(z < 3)
    def _():
        for f in range(8):
            greet(24 + f)

    @pl.when(z == 3)
    def _():
        for peer in lines:
            pl.semaphore_signal(barrier, inc=1, device_id={"freq": peer}, device_id_type=MESH)

    w = weight[...]
    root = jnp.sqrt(w)
    low = iota((1, 128), 1) < 64
    half = jnp.where(low, 1.0, -1.0).astype(F32)

    def split(s, hook):
        if s >= FIRST:
            load(s).wait()
        for c in range(3):
            if c == 1:
                hook()
            span = pl.ds(c * 1024, 1024)
            for part in range(2):
                for r in range(0, 64, 16):
                    y = (first[s, part, c, pl.ds(r, 16)] if s < FIRST else xbuf[s - FIRST, part, c, pl.ds(r, 16)]) * root
                    hi = y.astype(BF16)
                    lo = (y - hi.astype(F32)).astype(BF16)
                    ybuf[s][pl.ds(part * 64 + r, 16), span] = hi
                    ybuf[s][pl.ds(128 + part * 64 + r, 16), span] = lo

    def product(s):
        total = None
        for k in range(2):
            both = ybuf[s][:, pl.ds(k * 1536, 1536)]
            m = lax.dot_general(both, both, (((1,), (1,)), ((), ())), preferred_element_type=F32)
            m = (m[:128, :128] + m[128:, 128:]) + (m[:128, 128:] + m[128:, :128])
            total = m if total is None else total + m
        return total

    def packed(m):
        top, bottom = m[:64], m[64:]
        straight = top + half * pltpu.roll(bottom, 64, 1)
        swapped = pltpu.roll(top, 64, 1) - half * bottom
        row = iota((64, 128), 0)
        col = iota((64, 128), 1) % 64
        upper = jnp.where(low == (col >= row), straight, swapped)
        return jnp.where(low, upper[:32], upper[32:])

    def send_product(s):
        return pltpu.make_async_remote_copy(
            src_ref=pbuf.at[s], dst_ref=rbuf.at[own], send_sem=ps_sem.at[s], recv_sem=pr_sem.at[own],
            device_id={"pts": goal + freq[s]}, device_id_type=MESH)

    def take_product(at):
        return pltpu.make_async_remote_copy(
            src_ref=pbuf.at[0], dst_ref=rbuf.at[at], send_sem=ps_sem.at[0], recv_sem=pr_sem.at[at],
            device_id={"pts": goal + freq[0]}, device_id_type=MESH)

    def send_row():
        return pltpu.make_async_remote_copy(
            src_ref=gbuf, dst_ref=rbuf.at[8 + z], send_sem=gs_sem.at[0], recv_sem=pr_sem.at[8 + z],
            device_id={"pts": 24 + own}, device_id_type=MESH)

    before = None

    def passed(s):
        if not s:
            return
        pbuf[s - 1] = packed(before)
        if s == HELLO:
            pl.semaphore_wait(barrier, 7 + 27 * top)

            @pl.when(z == 3)
            def _():
                for peer in (0, 8, 16):
                    pl.semaphore_signal(
                        ready, inc=1, device_id={"pts": peer + own}, device_id_type=MESH)
        for k in range(s) if s == HELLO else [s - 1] if s > HELLO else []:
            send_product(k).start()

    for s in range(8):
        split(s, lambda: passed(s))
        before = product(s)
    pbuf[7] = packed(before)

    def send_trace(i):
        return pltpu.make_async_remote_copy(
            src_ref=tbuf.at[line], dst_ref=tbuf.at[line], send_sem=ts_sem.at[i], recv_sem=tr_sem.at[line],
            device_id={"freq": lines[i]}, device_id_type=MESH)

    def take_trace(i):
        return pltpu.make_async_remote_copy(
            src_ref=tbuf.at[line], dst_ref=tbuf.at[lines[i]], send_sem=ts_sem.at[i], recv_sem=tr_sem.at[lines[i]],
            device_id={"freq": lines[i]}, device_id_type=MESH)

    def send_basis(i):
        return pltpu.make_async_remote_copy(
            src_ref=vbuf.at[own], dst_ref=vbuf.at[own], send_sem=vs_sem.at[i], recv_sem=vr_sem.at[own],
            device_id={"pts": everyone[i]}, device_id_type=MESH)

    def take_basis(s):
        return pltpu.make_async_remote_copy(
            src_ref=vbuf.at[own], dst_ref=vbuf.at[freq[s]], send_sem=vs_sem.at[0], recv_sem=vr_sem.at[freq[s]],
            device_id={"pts": 24 + freq[s]}, device_id_type=MESH)

    def send_aux(i):
        return pltpu.make_async_remote_copy(
            src_ref=abuf.at[own], dst_ref=abuf.at[own], send_sem=as_sem.at[i], recv_sem=ar_sem.at[own],
            device_id={"pts": everyone[i]}, device_id_type=MESH)

    def take_aux(s):
        return pltpu.make_async_remote_copy(
            src_ref=abuf.at[own], dst_ref=abuf.at[freq[s]], send_sem=as_sem.at[0], recv_sem=ar_sem.at[freq[s]],
            device_id={"pts": 24 + freq[s]}, device_id_type=MESH)

    def applied(vectors):
        pieces = []
        for v in vectors:
            pieces.extend(split3(v))
        while len(pieces) % 2:
            pieces.append(jnp.zeros((8, 128), F32))
        left = jnp.concatenate(pieces, axis=0).astype(BF16)
        out = jnp.dot(jnp.concatenate([left, left], axis=1), rmat[...], preferred_element_type=F32)
        results = []
        for i in range(len(vectors)):
            parts = [out[24 * i + 8 * k : 24 * i + 8 * k + 8] for k in range(3)]
            small = (parts[2][:, :128] + parts[0][:, 128:]) + (parts[1][:, 128:] + parts[2][:, 128:])
            results.append(parts[0][:, :128] + (parts[1][:, :128] + small))
        return results


    @pl.when(z < 3)
    def _():
        total = pbuf[7]
        for s in range(7):
            take_product(freq[s]).wait_recv()
            total = total + rbuf[freq[s]]
        gbuf[...] = total
        pl.semaphore_wait(ready, 1)
        send_row().start()
        send_row().wait_send()

    @pl.when(z == 3)
    def _():
        total = pbuf[7]
        for s in range(7):
            take_product(freq[s]).wait_recv()
            total = total + rbuf[freq[s]]
        for at in (8, 9, 10):
            take_product(at).wait_recv()
            total = total + rbuf[at]
        gram = total * (1.0 / 98304.0)
        turned = pltpu.roll(gram, 64, 1)
        upper = jnp.concatenate([jnp.where(low, gram, turned), jnp.where(low, turned, gram)], axis=0)
        flipped = jnp.concatenate([upper, upper], axis=0).T[:64]
        row = iota((64, 128), 0)
        col = iota((64, 128), 1) % 64
        real = jnp.where(col >= row, upper, flipped)
        imag = jnp.where(col < row, upper, jnp.where(col > row, -flipped, 0.0))
        full = jnp.concatenate([jnp.where(low, real, -imag), jnp.where(low, imag, real)], axis=0)
        r0, r1, r2 = split3(full)
        rmat[pl.ds(0, 128), pl.ds(0, 128)] = r0.astype(BF16)
        rmat[pl.ds(128, 128), pl.ds(0, 128)] = r1.astype(BF16)
        rmat[pl.ds(0, 128), pl.ds(128, 128)] = r2.astype(BF16)
        rmat[pl.ds(128, 128), pl.ds(128, 128)] = jnp.zeros((128, 128), BF16)

        diag = jnp.where((col == row) & low, upper, 0.0)
        trace = jnp.sum(jnp.sum(diag, axis=1, keepdims=True), axis=0, keepdims=True)
        tbuf[line] = jnp.broadcast_to(trace, (8, 128))
        for i in range(3):
            send_trace(i).start()

        rank = iota((8, 128), 0)
        v = jnp.concatenate([start[0, own], start[1, own]], axis=1)
        iv = pltpu.roll(v, 64, 1) * -half
        scale = None
        zv, wv = v, iv
        for step in range(ITERS):
            zv, wv = applied([zv, wv])
            if scale is not None:
                zv, wv = zv * scale, wv * scale
            scale = jnp.zeros((8, 128), F32)
            for j in range(8):
                zj = jnp.broadcast_to(zv[j : j + 1], (8, 128))
                wj = jnp.broadcast_to(wv[j : j + 1], (8, 128))
                dot_real = jnp.broadcast_to(jnp.sum(zj * zv, axis=1, keepdims=True), (8, 128))
                norm = jnp.broadcast_to(dot_real[j : j + 1], (8, 128))
                factor = lax.rsqrt(norm * (1.0 / 64) + 1e-06)
                scale = jnp.where(rank == j, factor, scale)
                if j < 7:
                    dot_imag = jnp.broadcast_to(jnp.sum(wj * zv, axis=1, keepdims=True), (8, 128))
                    inverse = jnp.where(rank > j, factor * factor * (1.0 / 64), 0.0)
                    coef_real = dot_real * inverse
                    coef_imag = dot_imag * inverse
                    zv, wv = (
                        zv - (coef_real * zj + coef_imag * wj),
                        wv - (coef_real * wj - coef_imag * zj),
                    )
        (out,) = applied([zv])
        v = zv * scale
        vbuf[own] = v
        for i in range(31):
            send_basis(i).start()

        rayleigh = jnp.sum(v * (out * scale), axis=1, keepdims=True) * (1.0 / 64)
        spread = jnp.sum(jnp.where(rank == iota((8, 128), 1), rayleigh, 0.0), axis=0, keepdims=True)
        for i in (1, 2, 0):
            take_trace(i).wait_recv()
        group = (tbuf[0] + tbuf[1]) + (tbuf[2] + tbuf[3])
        abuf[own] = jnp.where(low, spread, group[:1])
        for i in range(31):
            send_aux(i).start()
        for i in range(3):
            send_trace(i).wait_send()

    undo = lax.rsqrt(w) * (1.0 / 64)

    for s in reversed(range(8)):
        if s < 7:
            take_basis(s).wait_recv()
        else:
            @pl.when(z < 3)
            def _():
                take_basis(7).wait_recv()
        vec = vbuf[freq[s]]
        other = pltpu.roll(vec, 64, 1)
        basis_out[0, freq[s]] = vec[:, :64]
        basis_out[1, freq[s]] = other[:, :64]
        left = jnp.concatenate([vec * half, other], axis=0)
        left_hi = left.astype(BF16)
        left_lo = (left - left_hi.astype(F32)).astype(BF16)
        left = jnp.concatenate([left_hi, left_lo], axis=0)
        left = jnp.concatenate([left, left], axis=1)
        for k in range(6):
            c, at = k // 2, k % 2 * 512
            out = jnp.dot(left, ybuf[s][:, pl.ds(k * 512, 512)], preferred_element_type=F32)
            out = (out[:16] + out[16:]) * undo[:, at : at + 512]
            modes_out[0, freq[s], c, :, pl.ds(at, 512)] = out[:8]
            modes_out[1, freq[s], c, :, pl.ds(at, 512)] = out[8:]

    for s in range(7):
        take_aux(s).wait_recv()

    @pl.when(z < 3)
    def _():
        take_aux(7).wait_recv()

    total = jnp.zeros((1, 8), F32)
    for f in range(8):
        total = total + abuf[f, :, 64:72]
    for f in range(8):
        spec_out[pl.ds(f, 1), :] = abuf[f, :, :8] * 2048.0 / total

    for s in range(7):
        send_product(s).wait_send()

    @pl.when(z == 3)
    def _():
        for i in range(31):
            send_basis(i).wait_send()
            send_aux(i).wait_send()


def writer(basis_in, spec_in, modes_in, basis_out, spec_out, modes_out, sem):
    copies = [
        pltpu.make_async_copy(modes_in.at[part, pl.ds(4 * i, 4)], modes_out.at[part, pl.ds(4 * i, 4)], sem.at[2 * part + i])
        for part in range(2) for i in range(2)
    ] + [
        pltpu.make_async_copy(basis_in, basis_out, sem.at[4]),
        pltpu.make_async_copy(spec_in, spec_out, sem.at[5]),
    ]
    for copy in copies:
        copy.start()
    for copy in copies:
        copy.wait()


def per_device(data, quad_weight, basis):
    data = jnp.transpose(data, (0, 1, 3, 2, 4))
    basis = jnp.transpose(basis, (0, 1, 3, 2))
    vmem = pl.BlockSpec(memory_space=pltpu.VMEM)
    hbm = pl.BlockSpec(memory_space=pltpu.HBM)
    dma = pltpu.SemaphoreType.DMA
    shapes = (
        jax.ShapeDtypeStruct((2, 8, 8, 64), F32),
        jax.ShapeDtypeStruct((8, 8), F32),
        jax.ShapeDtypeStruct((2, 8, 3, 8, 1024), F32),
    )
    first = pl.pallas_call(
        opening,
        out_shape=jax.ShapeDtypeStruct((FIRST, 2, 3, 64, 1024), F32),
        in_specs=[hbm],
        out_specs=vmem,
        scratch_shapes=[dma((FIRST,))],
        compiler_params=pltpu.CompilerParams(vmem_limit_bytes=48 * 1024 * 1024),
        cost_estimate=pl.CostEstimate(flops=10**9, bytes_accessed=6 * 10**6, transcendentals=0),
        name="opening",
    )(data)
    results = pl.pallas_call(
        kernel,
        out_shape=shapes,
        in_specs=[hbm, vmem, vmem, vmem],
        out_specs=(vmem, vmem, vmem),
        scratch_shapes=[
            pltpu.VMEM((8 - FIRST, 2, 3, 64, 1024), F32),
            pltpu.VMEM((8, 32, 128), F32),
            pltpu.VMEM((11, 32, 128), F32),
            pltpu.VMEM((32, 128), F32),
            pltpu.VMEM((4, 8, 128), F32),
            pltpu.VMEM((8, 8, 128), F32),
            pltpu.VMEM((8, 1, 128), F32),
            pltpu.VMEM((256, 256), BF16),
            dma((8,)), dma((8,)), dma((11,)), dma((1,)),
            dma((3,)), dma((4,)), dma((31,)), dma((8,)), dma((31,)), dma((8,)),
            pltpu.SemaphoreType.REGULAR,
            *[pltpu.VMEM((256, 3072), BF16) for _ in range(8)],
        ],
        compiler_params=pltpu.CompilerParams(
            collective_id=0, has_side_effects=True, vmem_limit_bytes=48 * 1024 * 1024
        ),
        name="spod",
    )(data, quad_weight.reshape(1, -1), basis, first)
    basis_out, spectrum, modes = pl.pallas_call(
        writer,
        out_shape=shapes,
        in_specs=[vmem, vmem, vmem],
        out_specs=(hbm, hbm, hbm),
        scratch_shapes=[dma((6,))],
        compiler_params=pltpu.CompilerParams(vmem_limit_bytes=4 * 1024 * 1024),
        name="writer",
    )(*results)
    return (
        jnp.transpose(basis_out, (0, 1, 3, 2)),
        spectrum,
        jnp.transpose(modes, (0, 1, 3, 2, 4)),
    )


def solution(mesh):
    in_specs = (P(None, "freq", None, None, "pts"), P("pts"), P(None, "freq", None, None))
    out_specs = (P(None, "freq", None, None), P("freq", None), P(None, "freq", None, None, "pts"))
    return jax.shard_map(
        per_device, mesh=mesh, in_specs=in_specs, out_specs=out_specs, check_vma=False
    )
```
